32 devices in a mesh: win: 16 (over z, y, core), head: 2 (over x).
Axes of the slice: x: 2, y: 2, z: 4, core: 2. Of those that a mesh axis runs over, the one named last changes fastest.
Arguments:
- qkv: bfloat16 [3, 16, 96, 48, 1024], P(None, 'win', 'head'), may hold values from -10 to 10
Outputs:
- attended: bfloat16 [16, 96, 48, 1024], P('win', 'head')
The draws below stay inside these ranges and needn't reach their ends.
All inputs are finite; a program needn't handle non-finite values.
Results may differ from the reference program's by a relative error of at most 0.0047.
Values may be sent and summed in bfloat16 or wider, within the bound.
A program may use at most 192 MiB of HBM per device.

```python
import math
import jax
import jax.numpy as jnp
from jax import lax

HEADS = 8
HEAD_DIM = 128
WIN = 48
LAT_WIN = 4
ROWS = 192
HALF_ROWS = 96
LON_BANDS = 8


def draw_qkv(key, part):
    channels = HEADS * HEAD_DIM
    blocks = 2 * LON_BANDS
    full_shape = (3, blocks, HALF_ROWS, WIN, channels)
    key_base = jax.random.fold_in(jax.random.fold_in(key, 7), 0)
    values = jnp.clip(jax.random.normal(key_base, full_shape, jnp.float32), -6.0, 6.0)
    return values.astype(jnp.bfloat16)


def setup_inputs(seed: int = 0) -> dict:
    seeds = jax.random.split(jax.random.key(seed), 2)
    qkv = draw_qkv(jax.random.fold_in(seeds[1], 71), 0)
    return {"qkv": qkv}


def attend(queries, keys, values, labels_query, labels_key):
    score_scale = 1.0 / math.sqrt(queries.shape[-1])
    scores = jnp.einsum('qhd,khd->hqk', queries.astype(jnp.float32), keys.astype(jnp.float32)) * score_scale
    allowed = labels_query[:, None] == labels_key[None, :]
    scores = jnp.where(allowed[None], scores, -jnp.inf)
    row_max = lax.optimization_barrier(jnp.max(scores, axis=-1, keepdims=True))
    weights = jnp.exp(scores - row_max)
    row_total = lax.optimization_barrier(jnp.sum(weights, axis=-1, keepdims=True))
    rounded = lax.optimization_barrier(weights.astype(jnp.bfloat16)).astype(jnp.float32)
    mixture = jnp.einsum('hqk,khd->qhd', rounded, values.astype(jnp.float32))
    return (mixture / jnp.transpose(row_total, (1, 0, 2))).astype(jnp.bfloat16)

def reference(qkv):
    half_cols = WIN // 2
    channels = HEADS * HEAD_DIM
    bands = qkv.reshape(3, LON_BANDS, ROWS, WIN, channels)
    rolled_rows = jnp.roll(jnp.arange(ROWS, dtype=jnp.int32), -half_cols)
    row_labels = (rolled_rows < half_cols).astype(jnp.int32)
    label_parts = jnp.broadcast_to(row_labels.reshape(LAT_WIN, WIN, 1), (LAT_WIN, WIN, WIN)).reshape(LAT_WIN, WIN * WIN)

    def one_window(lon_index):
        east_index = ((lon_index + 1) % LON_BANDS).astype(jnp.int32)
        own_band = lax.dynamic_index_in_dim(bands, lon_index, 1, keepdims=False)
        east_band = lax.dynamic_index_in_dim(bands, east_index, 1, keepdims=False)
        window = jnp.concatenate([own_band[:, :, half_cols:], east_band[:, :, :half_cols]], axis=2)
        window = jnp.roll(window, -half_cols, axis=1)
        window_parts = window.reshape(3, LAT_WIN, WIN * WIN, HEADS, HEAD_DIM)

        def one_band(pieces):
            window_part, label_part = pieces
            return attend(window_part[0], window_part[1], window_part[2], label_part, label_part)
        result = lax.map(one_band, (jnp.moveaxis(window_parts, 1, 0), label_parts))
        result = result.reshape(ROWS, WIN, channels)
        return jnp.roll(result, half_cols, axis=0)
    outputs = lax.map(one_window, jnp.arange(LON_BANDS, dtype=jnp.int32))
    joined = jnp.concatenate([jnp.roll(outputs[:, :, half_cols:], 1, axis=0), outputs[:, :, :half_cols]], axis=2)
    return joined.reshape(2 * LON_BANDS, HALF_ROWS, WIN, channels)
```

```python
import functools
import math

import jax
import jax.numpy as jnp
from jax import lax
from jax.experimental import pallas as pl
from jax.experimental.pallas import tpu as pltpu
from jax.sharding import PartitionSpec as P

HEAD_DIM = 128


def from_behind(shard, axis, by):
    count = lax.axis_size(axis)
    return lax.ppermute(shard, axis, [(i, (i + by) % count) for i in range(count)])


def partner(value, axis, apart):
    mask = 2**apart
    pairs = [(source, source ^ mask) for source in range(lax.axis_size(axis))]
    return lax.ppermute(value, axis, pairs)


def attend(queries, keys, values, labels_query, labels_key):
    query_count, head_count, head_width = queries.shape
    block_rows = math.gcd(query_count, 576)
    score_scale = 1.0 / math.sqrt(head_width)

    def one_block(pieces):
        query_block, label_block = pieces
        scores = (
            jnp.einsum("qhd,khd->hqk", query_block, keys, preferred_element_type=jnp.float32)
            * score_scale
        )
        allowed = label_block[:, None] == labels_key[None, :]
        scores = jnp.where(allowed[None], scores, -jnp.inf)
        row_max = jnp.max(scores, axis=-1, keepdims=True)
        weights = jnp.exp(scores - row_max)
        row_total = jnp.sum(weights, axis=-1, keepdims=True)
        mixture = jnp.einsum(
            "hqk,khd->qhd", weights.astype(jnp.bfloat16), values, preferred_element_type=jnp.float32
        )
        return (mixture / jnp.transpose(row_total, (1, 0, 2))).astype(jnp.bfloat16)

    query_blocks = queries.reshape(query_count // block_rows, block_rows, head_count, head_width)
    label_blocks = labels_query.reshape(query_count // block_rows, block_rows)
    return lax.map(one_block, (query_blocks, label_blocks)).reshape(
        query_count, head_count, head_width
    )


def window_attention(window, labels):
    row_count, side_cells, channels = (window.shape[1], window.shape[2], window.shape[3])
    head_count = channels // HEAD_DIM
    window_parts = window.reshape(
        3, row_count // side_cells, side_cells * side_cells, head_count, HEAD_DIM
    )
    label_parts = labels.reshape(row_count // side_cells, side_cells * side_cells)
    outputs = []
    for window_row in range(row_count // side_cells):
        outputs.append(
            attend(
                window_parts[0, window_row],
                window_parts[1, window_row],
                window_parts[2, window_row],
                label_parts[window_row],
                label_parts[window_row],
            )
        )
    return jnp.stack(outputs).reshape(row_count, side_cells, channels)


def general_body(qkv):
    side_cells = qkv.shape[3]
    half_cols = side_cells // 2
    tokens = qkv[:, 0]
    arrived = from_behind(tokens[:, :, :half_cols], "win", -2)
    tokens = jnp.concatenate([tokens[:, :, half_cols:], arrived], axis=2)
    head_view = lax.all_to_all(tokens, "head", split_axis=3, concat_axis=1, tiled=True)
    half_rows = head_view.shape[1]
    crossing = partner(head_view[:, :half_cols], "win", 0)
    extended = jnp.concatenate([head_view[:, half_cols:], crossing], axis=1)
    lat_half = lax.axis_index("win") % 2
    row_index = jnp.arange(half_rows, dtype=jnp.int32)[:, None]
    wrapped = jnp.logical_and(lat_half == 1, row_index >= half_rows - half_cols)
    labels = jnp.broadcast_to(jnp.where(wrapped, 1, 0).astype(jnp.int32), (half_rows, side_cells))
    result = window_attention(extended, labels)
    returned = partner(result[half_rows - half_cols :], "win", 0)
    row_fixed = jnp.concatenate([returned, result[: half_rows - half_cols]], axis=0)
    restored = lax.all_to_all(row_fixed, "head", split_axis=0, concat_axis=2, tiled=True)
    from_west = from_behind(restored[:, half_cols:], "win", 2)
    restored = jnp.concatenate([from_west, restored[:, :half_cols]], axis=1)
    return restored[None]


MESH = pl.DeviceIdType.MESH


def scan_blocks(block_rows, count, q_all, k_all, v_all, o_all, scores_a, scores_b, max_a, max_b):
    width = q_all.shape[1]
    factor = math.log2(math.e) / math.sqrt(width)
    keys = pl.ds(0, count)
    blocks = count // block_rows

    def rows_of(block):
        return pl.ds(pl.multiple_of(block * block_rows, block_rows), block_rows)

    def score(block, scores, row_max):
        s = lax.dot_general(
            q_all[rows_of(block), :],
            k_all[keys, :],
            (((1,), (1,)), ((), ())),
            preferred_element_type=jnp.float32,
        )
        scores[:, keys] = s
        row_max[...] = jnp.broadcast_to(jnp.max(s, axis=1, keepdims=True) * factor, row_max.shape)

    def mix(block, scores, row_max):
        top = row_max[:, pl.ds(0, 1)]
        weights = jnp.exp2(scores[:, keys] * factor - top)
        mixture = jnp.dot(
            weights.astype(jnp.bfloat16), v_all[keys, :], preferred_element_type=jnp.float32
        )
        o_all[rows_of(block), :] = (mixture[:, :width] / mixture[:, width:]).astype(jnp.bfloat16)

    score(0, scores_a, max_a)

    def pair(step, carry):
        score(2 * step + 1, scores_b, max_b)
        mix(2 * step, scores_a, max_a)
        score(jnp.minimum(2 * step + 2, blocks - 1), scores_a, max_a)
        mix(2 * step + 1, scores_b, max_b)
        return carry

    lax.fori_loop(0, blocks // 2, pair, 0)


def window_kernel(axis_heads, bands, qkv, out, tok, res, *refs):
    q_all, k_all, v_all, o_all, scores_a, scores_b, max_a, max_b = refs[:8]
    in_send, in_recv, own_sem, out_send, out_recv = refs[8:]
    heads, half, width = tok.shape[0], tok.shape[3], tok.shape[5]
    part = half * half
    block_rows = part // 3
    win = lax.axis_index("win")
    rows_at = (win % 2) * axis_heads + lax.axis_index("head")
    band = win // 2
    first = (rows_at == 0).astype(jnp.int32)
    last = (rows_at == 2 * axis_heads - 1).astype(jnp.int32)

    def device(rows, columns):
        row = rows_at + rows
        column = (band + columns + bands) % bands
        return {"win": column * 2 + row // axis_heads, "head": row % axis_heads}

    barrier = pltpu.get_barrier_semaphore()

    def greet(rows):
        for columns in (-1, 0, 1):
            if rows or columns:
                pl.semaphore_signal(
                    barrier, inc=1, device_id=device(rows, columns), device_id_type=MESH
                )

    greet(0)

    @pl.when(first == 0)
    def _():
        greet(-1)

    @pl.when(last == 0)
    def _():
        greet(1)

    @pl.when(first + last == 0)
    def _():
        pl.semaphore_wait(barrier, 8)

    @pl.when(first + last != 0)
    def _():
        pl.semaphore_wait(barrier, 5)

    def remote(source, target, sent, received, to):
        return pltpu.make_async_remote_copy(
            src_ref=source,
            dst_ref=target,
            send_sem=sent,
            recv_sem=received,
            device_id=to,
            device_id_type=MESH,
        )

    low, high = pl.ds(0, half), pl.ds(half, half)

    class Head:
        def __init__(self, h):
            side = h % 2
            main = pl.ds((1 - side) * half, half)
            other = pl.ds(side * half, half)
            step = 2 * side - 1
            lanes = pl.ds(pl.multiple_of(h * width, width), width)
            self.h = h
            self.solo = first * (1 - side) + last * side
            self.joined = 1 - last * (1 - side) - first * side
            s, r, o, g = in_send.at[h], in_recv.at[h], out_send.at[h], out_recv.at[h]
            self.far = lambda: remote(
                qkv.at[:, 0, other, low, lanes], tok.at[h, 5], s.at[0], r.at[0], device(0, -1)
            )
            self.near = lambda: remote(
                qkv.at[:, 0, main, low, lanes], tok.at[h, 1], s.at[1], r.at[1], device(0, -1)
            )
            self.cross = lambda: remote(
                qkv.at[:, 0, other, high, lanes], tok.at[h, 2], s.at[2], r.at[2], device(step, 0)
            )
            self.relay = lambda: remote(tok.at[h, 5], tok.at[h, 3], s.at[3], r.at[3], device(step, 0))
            self.own = lambda: pltpu.make_async_copy(
                qkv.at[:, 0, main, high, lanes], tok.at[h, 0], own_sem.at[h, 0]
            )
            self.own_far = lambda: pltpu.make_async_copy(
                qkv.at[:, 0, other, high, lanes], tok.at[h, 4], own_sem.at[h, 1]
            )
            self.main, self.other, self.lanes = main, other, lanes
            self.back_near = lambda: remote(
                res.at[h, 1], out.at[0, main, low, lanes], o.at[0], g.at[0], device(0, 1)
            )
            self.back_cross = lambda: remote(
                res.at[h, 2], out.at[0, other, high, lanes], o.at[1], g.at[1], device(-step, 0)
            )
            self.back_corner = lambda: remote(
                res.at[h, 3], out.at[0, other, low, lanes], o.at[2], g.at[2], device(-step, 1)
            )
            self.back_far = lambda: remote(
                res.at[h, 5], out.at[0, other, low, lanes], o.at[3], g.at[2], device(0, 1)
            )

    def when(flag):
        return pl.when(flag != 0)

    def start_local(h, carry):
        head = Head(h)
        head.own().start()

        @when(head.solo)
        def _():
            head.own_far().start()

        return carry

    def start_cross(h):
        head = Head(h)

        @when(1 - head.solo)
        def _():
            head.cross().start()

    def load(h, slot, place):
        rows = pl.ds(place * part, part)
        q_all[rows, :] = tok[h, slot, 0].reshape(part, width)
        k_all[rows, :] = tok[h, slot, 1].reshape(part, width)
        v_all[rows, pl.ds(0, width)] = tok[h, slot, 2].reshape(part, width)

    def store(h, slot, place, rows=None):
        quarter = o_all[pl.ds(place * part, part), :].reshape(half, half, width)
        if rows is None:
            res[h, slot] = quarter
        else:
            out[0, rows, high, Head(h).lanes] = quarter

    scan = functools.partial(scan_blocks, block_rows)
    work = (q_all, k_all, v_all, o_all, scores_a, scores_b, max_a, max_b)

    def compute(h):
        head = Head(h)
        head.own().wait()
        head.near().wait_recv()

        @when(head.joined)
        def _():
            head.cross().wait_recv()
            head.relay().wait_recv()
            for slot in range(4):
                load(h, slot, slot)
            scan(4 * part, *work)
            for slot in range(4):
                store(h, slot, slot, None if slot else head.main)
            head.back_cross().start()

        @when(head.solo)
        def _():
            head.own_far().wait()

        @when(head.solo + 1 - head.joined)
        def _():
            base = 4 * head.joined
            for place in range(2):
                load(h, base + place, place)
            scan(2 * part, *work)
            own_rows = pl.ds(jnp.where(head.joined == 1, h % 2, 1 - h % 2) * half, half)
            for place in range(2):
                store(h, base + place, place, None if place else own_rows)

    def send_back(h, carry):
        head = Head(h)
        head.back_near().start()

        @when(head.solo)
        def _():
            head.back_far().start()

        return carry

    def send_corner(h, carry):
        head = Head(h)

        @when(head.joined)
        def _():
            head.back_corner().start()

        return carry

    def finish(h, carry):
        head = Head(h)
        head.back_near().wait()

        @when(head.solo)
        def _():
            head.back_far().wait_send()

            head.back_far().wait_recv()

        @when(1 - head.solo)
        def _():
            head.cross().wait_send()
            head.relay().wait_send()
            head.back_cross().wait_recv()
            head.back_corner().wait_recv()

        @when(head.joined)
        def _():
            head.back_cross().wait_send()
            head.back_corner().wait_send()

        return carry

    def step(h, carry):
        head = Head(h)
        @pl.when(h + 1 == heads)
        def _():
            lax.fori_loop(0, heads - 2, send_back, 0)

        head.far().wait()

        @when(1 - head.solo)
        def _():
            head.relay().start()

        @pl.when(h + 1 < heads)
        def _():
            Head(h + 1).near().start()
            start_cross(h + 1)

        head.near().wait_send()

        @pl.when(h + 2 < heads)
        def _():
            Head(h + 2).far().start()

        @pl.when(h + 1 == heads)
        def _():
            lax.fori_loop(0, heads - 2, send_corner, 0)

        @pl.when(h > 0)
        def _():
            compute(h - 1)

        return carry

    Head(0).far().start()
    Head(0).near().start()
    Head(1).far().start()
    start_cross(0)
    lax.fori_loop(0, heads, start_local, 0)
    v_all[:, pl.ds(width, width)] = jnp.ones((4 * part, width), jnp.bfloat16)
    lax.fori_loop(0, heads, step, 0)
    send_back(heads - 2, 0)
    send_corner(heads - 2, 0)
    compute(heads - 1)
    send_back(heads - 1, 0)
    send_corner(heads - 1, 0)
    lax.fori_loop(0, heads, finish, 0)


PUTS = 8


def put_kernel(source, target, sems):
    rows = source.shape[1] // PUTS

    def put(index):
        at = pl.ds(index * rows, rows)
        return pltpu.make_async_copy(source.at[0, at], target.at[0, at], sems.at[index])

    for index in range(PUTS):
        put(index).start()
    for index in range(PUTS):
        put(index).wait()


def window_body(axis_heads, bands, qkv):
    side, channels = qkv.shape[3], qkv.shape[4]
    half = side // 2
    part = half * half
    tokens = 4 * part
    heads = channels // HEAD_DIM
    block_rows = part // 3
    vmem, dma = pltpu.VMEM, pltpu.SemaphoreType.DMA
    bf16, f32 = jnp.bfloat16, jnp.float32
    gathered = pl.pallas_call(
        functools.partial(window_kernel, axis_heads, bands),
        in_specs=[pl.BlockSpec(memory_space=pl.ANY)],
        out_specs=pl.BlockSpec(memory_space=vmem),
        out_shape=vmem((1, side, side, channels), bf16),
        scratch_shapes=[
            vmem((heads, 6, 3, half, half, HEAD_DIM), bf16),
            vmem((heads, 6, half, half, HEAD_DIM), bf16),
            vmem((tokens, HEAD_DIM), bf16),
            vmem((tokens, HEAD_DIM), bf16),
            vmem((tokens, 2 * HEAD_DIM), bf16),
            vmem((tokens, HEAD_DIM), bf16),
            vmem((block_rows, tokens), f32),
            vmem((block_rows, tokens), f32),
            vmem((block_rows, HEAD_DIM), f32),
            vmem((block_rows, HEAD_DIM), f32),
            dma((heads, 4)),
            dma((heads, 4)),
            dma((heads, 2)),
            dma((heads, 4)),
            dma((heads, 3)),
        ],
        compiler_params=pltpu.CompilerParams(
            collective_id=0, has_side_effects=True, vmem_limit_bytes=50 * 2**20
        ),
    )(qkv)
    return pl.pallas_call(
        put_kernel,
        in_specs=[pl.BlockSpec(memory_space=vmem)],
        out_specs=pl.BlockSpec(memory_space=pl.ANY),
        out_shape=jax.ShapeDtypeStruct((1, side, side, channels), bf16),
        scratch_shapes=[dma((PUTS,))],
        compiler_params=pltpu.CompilerParams(vmem_limit_bytes=2**20),
    )(gathered)


def solution(mesh):
    in_specs = (P(None, "win", "head", None, None),)
    out_specs = P("win", "head", None, None)
    win_count, head_count = mesh.shape["win"], mesh.shape["head"]

    def body(qkv):
        if qkv.shape[2] == qkv.shape[3]:
            return window_body(head_count, win_count // 2, qkv)
        return general_body(qkv)

    return jax.shard_map(body, mesh=mesh, in_specs=in_specs, out_specs=out_specs, check_vma=False)
```

```python
import functools
import math

import jax
import jax.numpy as jnp
from jax import lax
from jax.experimental import pallas as pl
from jax.experimental.pallas import tpu as pltpu
from jax.sharding import PartitionSpec as P

HEAD_DIM = 128


def from_behind(shard, axis, by):
    count = lax.axis_size(axis)
    return lax.ppermute(shard, axis, [(i, (i + by) % count) for i in range(count)])


def partner(value, axis, apart):
    mask = 2**apart
    pairs = [(source, source ^ mask) for source in range(lax.axis_size(axis))]
    return lax.ppermute(value, axis, pairs)


def attend(queries, keys, values, labels_query, labels_key):
    query_count, head_count, head_width = queries.shape
    block_rows = math.gcd(query_count, 576)
    score_scale = 1.0 / math.sqrt(head_width)

    def one_block(pieces):
        query_block, label_block = pieces
        scores = (
            jnp.einsum("qhd,khd->hqk", query_block, keys, preferred_element_type=jnp.float32)
            * score_scale
        )
        allowed = label_block[:, None] == labels_key[None, :]
        scores = jnp.where(allowed[None], scores, -jnp.inf)
        row_max = jnp.max(scores, axis=-1, keepdims=True)
        weights = jnp.exp(scores - row_max)
        row_total = jnp.sum(weights, axis=-1, keepdims=True)
        mixture = jnp.einsum(
            "hqk,khd->qhd", weights.astype(jnp.bfloat16), values, preferred_element_type=jnp.float32
        )
        return (mixture / jnp.transpose(row_total, (1, 0, 2))).astype(jnp.bfloat16)

    query_blocks = queries.reshape(query_count // block_rows, block_rows, head_count, head_width)
    label_blocks = labels_query.reshape(query_count // block_rows, block_rows)
    return lax.map(one_block, (query_blocks, label_blocks)).reshape(
        query_count, head_count, head_width
    )


def window_attention(window, labels):
    row_count, side_cells, channels = (window.shape[1], window.shape[2], window.shape[3])
    head_count = channels // HEAD_DIM
    window_parts = window.reshape(
        3, row_count // side_cells, side_cells * side_cells, head_count, HEAD_DIM
    )
    label_parts = labels.reshape(row_count // side_cells, side_cells * side_cells)
    outputs = []
    for window_row in range(row_count // side_cells):
        outputs.append(
            attend(
                window_parts[0, window_row],
                window_parts[1, window_row],
                window_parts[2, window_row],
                label_parts[window_row],
                label_parts[window_row],
            )
        )
    return jnp.stack(outputs).reshape(row_count, side_cells, channels)


def general_body(qkv):
    side_cells = qkv.shape[3]
    half_cols = side_cells // 2
    tokens = qkv[:, 0]
    arrived = from_behind(tokens[:, :, :half_cols], "win", -2)
    tokens = jnp.concatenate([tokens[:, :, half_cols:], arrived], axis=2)
    head_view = lax.all_to_all(tokens, "head", split_axis=3, concat_axis=1, tiled=True)
    half_rows = head_view.shape[1]
    crossing = partner(head_view[:, :half_cols], "win", 0)
    extended = jnp.concatenate([head_view[:, half_cols:], crossing], axis=1)
    lat_half = lax.axis_index("win") % 2
    row_index = jnp.arange(half_rows, dtype=jnp.int32)[:, None]
    wrapped = jnp.logical_and(lat_half == 1, row_index >= half_rows - half_cols)
    labels = jnp.broadcast_to(jnp.where(wrapped, 1, 0).astype(jnp.int32), (half_rows, side_cells))
    result = window_attention(extended, labels)
    returned = partner(result[half_rows - half_cols :], "win", 0)
    row_fixed = jnp.concatenate([returned, result[: half_rows - half_cols]], axis=0)
    restored = lax.all_to_all(row_fixed, "head", split_axis=0, concat_axis=2, tiled=True)
    from_west = from_behind(restored[:, half_cols:], "win", 2)
    restored = jnp.concatenate([from_west, restored[:, :half_cols]], axis=1)
    return restored[None]


MESH = pl.DeviceIdType.MESH


def scan_blocks(block_rows, count, q_all, k_all, v_all, o_all, scores_a, scores_b, max_a, max_b):
    width = q_all.shape[1]
    factor = math.log2(math.e) / math.sqrt(width)
    keys = pl.ds(0, count)
    blocks = count // block_rows

    def rows_of(block):
        return pl.ds(pl.multiple_of(block * block_rows, block_rows), block_rows)

    def score(block, scores, row_max):
        s = lax.dot_general(
            q_all[rows_of(block), :],
            k_all[keys, :],
            (((1,), (1,)), ((), ())),
            preferred_element_type=jnp.float32,
        )
        scores[:, keys] = s
        row_max[...] = jnp.broadcast_to(jnp.max(s, axis=1, keepdims=True) * factor, row_max.shape)

    def mix(block, scores, row_max):
        top = row_max[:, pl.ds(0, 1)]
        weights = jnp.exp2(scores[:, keys] * factor - top)
        mixture = jnp.dot(
            weights.astype(jnp.bfloat16), v_all[keys, :], preferred_element_type=jnp.float32
        )
        o_all[rows_of(block), :] = (mixture[:, :width] / mixture[:, width:]).astype(jnp.bfloat16)

    score(0, scores_a, max_a)

    def pair(step, carry):
        score(2 * step + 1, scores_b, max_b)
        mix(2 * step, scores_a, max_a)
        score(jnp.minimum(2 * step + 2, blocks - 1), scores_a, max_a)
        mix(2 * step + 1, scores_b, max_b)
        return carry

    lax.fori_loop(0, blocks // 2, pair, 0)


def window_kernel(axis_heads, bands, qkv, out, tok, res, *refs):
    q_all, k_all, v_all, o_all, scores_a, scores_b, max_a, max_b = refs[:8]
    in_send, in_recv, own_sem, out_send, out_recv = refs[8:]
    heads, half, width = tok.shape[0], tok.shape[3], tok.shape[5]
    part = half * half
    block_rows = part // 3
    win = lax.axis_index("win")
    rows_at = (win % 2) * axis_heads + lax.axis_index("head")
    band = win // 2
    first = (rows_at == 0).astype(jnp.int32)
    last = (rows_at == 2 * axis_heads - 1).astype(jnp.int32)
    yields = (band % 2) * (band != bands - 1).astype(jnp.int32)

    def device(rows, columns):
        row = rows_at + rows
        column = (band + columns + bands) % bands
        return {"win": column * 2 + row // axis_heads, "head": row % axis_heads}

    barrier = pltpu.get_barrier_semaphore()

    def greet(rows, columns):
        pl.semaphore_signal(barrier, inc=1, device_id=device(rows, columns), device_id_type=MESH)

    greet(0, -1)
    greet(0, 1)

    @pl.when(first == 0)
    def _():
        greet(-1, 0)

    @pl.when(last == 0)
    def _():
        greet(1, 0)

    @pl.when(first + last == 0)
    def _():
        pl.semaphore_wait(barrier, 4)

    @pl.when(first + last != 0)
    def _():
        pl.semaphore_wait(barrier, 3)

    def remote(source, target, sent, received, to):
        return pltpu.make_async_remote_copy(
            src_ref=source,
            dst_ref=target,
            send_sem=sent,
            recv_sem=received,
            device_id=to,
            device_id_type=MESH,
        )

    low, high = pl.ds(0, half), pl.ds(half, half)

    class Head:
        def __init__(self, h):
            side = h % 2
            main = pl.ds((1 - side) * half, half)
            other = pl.ds(side * half, half)
            step = 2 * side - 1
            lanes = pl.ds(pl.multiple_of(h * width, width), width)
            self.h = h
            self.solo = first * (1 - side) + last * side
            self.joined = 1 - last * (1 - side) - first * side
            s, r, o, g = in_send.at[h], in_recv.at[h], out_send.at[h], out_recv.at[h]
            self.far = lambda: remote(
                qkv.at[:, 0, other, low, lanes], tok.at[h, 5], s.at[0], r.at[0], device(0, -1)
            )
            self.near = lambda: remote(
                qkv.at[:, 0, main, low, lanes], tok.at[h, 1], s.at[1], r.at[1], device(0, -1)
            )
            self.cross = lambda: remote(
                qkv.at[:, 0, other, high, lanes], tok.at[h, 2], s.at[2], r.at[2], device(step, 0)
            )
            self.relay = lambda: remote(tok.at[h, 5], tok.at[h, 3], s.at[3], r.at[3], device(step, 0))
            self.own = lambda: pltpu.make_async_copy(
                qkv.at[:, 0, main, high, lanes], tok.at[h, 0], own_sem.at[h, 0]
            )
            self.own_far = lambda: pltpu.make_async_copy(
                qkv.at[:, 0, other, high, lanes], tok.at[h, 4], own_sem.at[h, 1]
            )
            self.main, self.other, self.lanes = main, other, lanes
            self.back_near = lambda: remote(
                res.at[h, 1], out.at[0, main, low, lanes], o.at[0], g.at[0], device(0, 1)
            )
            self.back_cross = lambda: remote(
                res.at[h, 2], out.at[0, other, high, lanes], o.at[1], g.at[1], device(-step, 0)
            )
            self.back_corner = lambda: remote(
                res.at[h, 3], res.at[h, 5], o.at[2], g.at[3], device(-step, 0)
            )
            self.back_far = lambda: remote(
                res.at[h, 5], out.at[0, other, low, lanes], o.at[3], g.at[2], device(0, 1)
            )

    def when(flag):
        return pl.when(flag != 0)

    def start_local(h, carry):
        head = Head(h)
        head.own().start()

        @when(head.solo)
        def _():
            head.own_far().start()

        return carry

    def start_cross(h):
        head = Head(h)

        @when(1 - head.solo)
        def _():
            head.cross().start()

    def load(h, slot, place):
        rows = pl.ds(place * part, part)
        q_all[rows, :] = tok[h, slot, 0].reshape(part, width)
        k_all[rows, :] = tok[h, slot, 1].reshape(part, width)
        v_all[rows, pl.ds(0, width)] = tok[h, slot, 2].reshape(part, width)

    def store(h, slot, place, rows=None):
        quarter = o_all[pl.ds(place * part, part), :].reshape(half, half, width)
        if rows is None:
            res[h, slot] = quarter
        else:
            out[0, rows, high, Head(h).lanes] = quarter

    scan = functools.partial(scan_blocks, block_rows)
    work = (q_all, k_all, v_all, o_all, scores_a, scores_b, max_a, max_b)

    def compute(h):
        head = Head(h)
        head.own().wait()

        @when(1 - yields * (h == heads - 1).astype(jnp.int32))
        def _():
            head.near().wait_recv()

        @when(head.joined)
        def _():
            head.cross().wait_recv()
            head.relay().wait_recv()
            for slot in range(4):
                load(h, slot, slot)
            scan(4 * part, *work)
            for slot in range(4):
                store(h, slot, slot, None if slot else head.main)
            head.back_corner().start()
            head.back_cross().start()

        @when(head.solo)
        def _():
            head.own_far().wait()

        @when(head.solo + 1 - head.joined)
        def _():
            base = 4 * head.joined
            for place in range(2):
                load(h, base + place, place)
            scan(2 * part, *work)
            own_rows = pl.ds(jnp.where(head.joined == 1, h % 2, 1 - h % 2) * half, half)
            for place in range(2):
                store(h, base + place, place, None if place else own_rows)

    def send_far(h):
        head = Head(h)

        @when(1 - head.solo)
        def _():
            head.back_corner().wait_recv()

        head.back_far().start()

    def send_back(h, carry):
        Head(h).back_near().start()
        send_far(h)
        return carry

    def finish(h, carry):
        head = Head(h)
        head.back_near().wait()
        head.back_far().wait()

        @when(1 - head.solo)
        def _():
            head.cross().wait_send()
            head.relay().wait_send()
            head.back_cross().wait_recv()

        @when(head.joined)
        def _():
            head.back_cross().wait_send()
            head.back_corner().wait_send()

        return carry

    def step(h, carry):
        head = Head(h)
        head.far().wait()

        @when(1 - head.solo)
        def _():
            head.relay().start()

        @pl.when(h + 1 < heads)
        def _():
            Head(h + 1).near().start()
            start_cross(h + 1)

        head.near().wait_send()

        @pl.when(h + 2 < heads)
        def _():
            Head(h + 2).far().start()

        @pl.when(h + 1 == heads)
        def _():
            @when(yields)
            def _():
                head.near().wait_recv()

            lax.fori_loop(0, heads - EARLY, send_back, 0)

        @pl.when(h > 0)
        def _():
            compute(h - 1)

        return carry

    Head(0).far().start()
    Head(0).near().start()
    Head(1).far().start()
    start_cross(0)
    lax.fori_loop(0, heads, start_local, 0)
    v_all[:, pl.ds(width, width)] = jnp.ones((4 * part, width), jnp.bfloat16)
    lax.fori_loop(0, heads, step, 0)
    lax.fori_loop(heads - EARLY, heads - 2, send_back, 0)
    Head(heads - 2).back_near().start()
    compute(jnp.int32(heads - 1))
    send_far(heads - 2)
    send_back(heads - 1, 0)
    lax.fori_loop(0, heads, finish, 0)


PUTS = 8
EARLY = 4


def put_kernel(source, target, sems):
    rows = source.shape[1] // PUTS

    def put(index):
        at = pl.ds(index * rows, rows)
        return pltpu.make_async_copy(source.at[0, at], target.at[0, at], sems.at[index])

    for index in range(PUTS):
        put(index).start()
    for index in range(PUTS):
        put(index).wait()


def window_body(axis_heads, bands, qkv):
    side, channels = qkv.shape[3], qkv.shape[4]
    half = side // 2
    part = half * half
    tokens = 4 * part
    heads = channels // HEAD_DIM
    block_rows = part // 3
    vmem, dma = pltpu.VMEM, pltpu.SemaphoreType.DMA
    bf16, f32 = jnp.bfloat16, jnp.float32
    gathered = pl.pallas_call(
        functools.partial(window_kernel, axis_heads, bands),
        in_specs=[pl.BlockSpec(memory_space=pl.ANY)],
        out_specs=pl.BlockSpec(memory_space=vmem),
        out_shape=vmem((1, side, side, channels), bf16),
        scratch_shapes=[
            vmem((heads, 6, 3, half, half, HEAD_DIM), bf16),
            vmem((heads, 6, half, half, HEAD_DIM), bf16),
            vmem((tokens, HEAD_DIM), bf16),
            vmem((tokens, HEAD_DIM), bf16),
            vmem((tokens, 2 * HEAD_DIM), bf16),
            vmem((tokens, HEAD_DIM), bf16),
            vmem((block_rows, tokens), f32),
            vmem((block_rows, tokens), f32),
            vmem((block_rows, HEAD_DIM), f32),
            vmem((block_rows, HEAD_DIM), f32),
            dma((heads, 4)),
            dma((heads, 4)),
            dma((heads, 2)),
            dma((heads, 4)),
            dma((heads, 4)),
        ],
        compiler_params=pltpu.CompilerParams(
            collective_id=0, has_side_effects=True, vmem_limit_bytes=50 * 2**20
        ),
    )(qkv)
    return pl.pallas_call(
        put_kernel,
        in_specs=[pl.BlockSpec(memory_space=vmem)],
        out_specs=pl.BlockSpec(memory_space=pl.ANY),
        out_shape=jax.ShapeDtypeStruct((1, side, side, channels), bf16),
        scratch_shapes=[dma((PUTS,))],
        compiler_params=pltpu.CompilerParams(vmem_limit_bytes=2**20),
    )(gathered)


def solution(mesh):
    in_specs = (P(None, "win", "head", None, None),)
    out_specs = P("win", "head", None, None)
    win_count, head_count = mesh.shape["win"], mesh.shape["head"]

    def body(qkv):
        if qkv.shape[2] == qkv.shape[3]:
            return window_body(head_count, win_count // 2, qkv)
        return general_body(qkv)

    return jax.shard_map(body, mesh=mesh, in_specs=in_specs, out_specs=out_specs, check_vma=False)
```
